32 devices in a mesh: groups: 2 (over y), wide: 8 (over z, x), narrow: 2 (over core).
Axes of the slice: x: 2, y: 2, z: 4, core: 2. Of those that a mesh axis runs over, the one named last changes fastest.
Arguments:
- hidden_in: bfloat16 [6400, 1024], P(('groups', 'wide')), parts along dimension 0, may hold values from -6 to 6
- ffn_gain: bfloat16 [1024], replicated, may hold values from 0.5 to 1.5
- wi_gate: bfloat16 [1024, 2816], P('wide', 'narrow'), may hold values from -0.1875 to 0.1875
- wi_up: bfloat16 [1024, 2816], P('wide', 'narrow'), may hold values from -0.1875 to 0.1875
- wo_down: bfloat16 [2816, 1024], P('narrow', 'wide'), may hold values from -0.109375 to 0.109375
- final_gain: bfloat16 [1024], replicated, may hold values from 0.5 to 1.5
- key_w: bfloat16 [1024, 1024], P('wide', 'narrow'), may hold values from -0.1875 to 0.1875
- value_w: bfloat16 [1024, 1024], P('wide', 'narrow'), may hold values from -0.1875 to 0.1875
- query_w: bfloat16 [1024, 1024], P('wide', 'narrow'), may hold values from -8 to 8
- out_w: bfloat16 [1024, 1024], P('narrow', 'wide'), may hold values from -0.1875 to 0.1875
- dec_gain: bfloat16 [1024], replicated, may hold values from 0.5 to 1.5
- embed: bfloat16 [32128, 1024], P('wide'), may hold values from -6 to 6
- lengths: int32 [32], P(('groups', 'wide')), parts along dimension 0, may hold values from 40 to 200
- answer_ids: int32 [8, 32], P('groups'), parts along dimension 0, may hold values from 0 to 32127
Outputs:
- memory: bfloat16 [6400, 1024], P(('groups', 'wide')), parts along dimension 0
- decoded: bfloat16 [256, 1024], P('groups', 'narrow'), parts along dimension 0
The draws below stay inside these ranges and needn't reach their ends.
There are 2 independent parts, one for each index of `groups`. The reference program is written for one: setup_inputs(seed, part) draws one part's arguments, and reference() takes and returns one part's arrays. A program takes and returns all parts, laid end to end along the dimension named above; an argument that names none is the same for every part. Nothing has to cross between parts.
All inputs are finite; a program needn't handle non-finite values.
Results may differ from the reference program's by a relative error of at most 0.0095.
The reference program's roundings to bfloat16 on the way (of `enc_in`, `inner`, `embedded`, `dec_in`, `query` and `attended`) count: a program that leaves them out, or rounds other values in their place, can miss the bound.
Values may be sent and summed in bfloat16 or wider, within the bound.
A program may use at most 64 MiB of HBM per device.

```python
import math
import jax
import jax.numpy as jnp
from jax import lax

D = 1024
HEADS = 16
HEAD_DIM = 64
FF = 2816
VOCAB = 32128
SEG = 200
QUEST = 4
ANS = 32
PASSAGES = 16
TOKENS = 3200
PER_Q = 4
QROWS = 128


def draw_query_w(key, part):
    base = jax.random.normal(jax.random.fold_in(key, 11), (D, D), jnp.float32)
    picked = jax.random.permutation(jax.random.fold_in(key, 12), HEADS)[:2]
    column_head = jnp.arange(D, dtype=jnp.int32) // HEAD_DIM
    strengths = jnp.array([60.0, 100.0], jnp.float32)
    factor = jnp.ones((D,), jnp.float32)
    factor = jnp.where(column_head == picked[0], strengths[0], factor)
    factor = jnp.where(column_head == picked[1], strengths[1], factor)
    scaled = base * (factor / math.sqrt(D))[None, :]
    return jnp.clip(scaled, -8.0, 8.0).astype(jnp.bfloat16)


def set_ends(result, own_key, least, largest):
    place = [jax.random.randint(jax.random.fold_in(own_key, axis), (), 0, length) for axis, length in enumerate(result.shape)]
    longest = result.shape.index(max(result.shape))
    neighbour = place[:longest] + [(place[longest] + 1) % result.shape[longest]] + place[longest + 1:]
    return result.at[tuple(place)].set(least).at[tuple(neighbour)].set(largest)


def shard_levels(rng, shape, split, low, top_value):
    factor_of, own = 1.0, jax.random.fold_in(rng, 6)
    for axis_at, shards_of in split:
        heights = jnp.exp(jax.random.uniform(jax.random.fold_in(own, axis_at), (shards_of,), jnp.float32, low / len(split), top_value / len(split)))
        factor_of = factor_of * jnp.repeat(heights, shape[axis_at] // shards_of).reshape([-1 if axis == axis_at else 1 for axis in range(len(shape))])
    return factor_of


def normal_values(own_key, dims, width, reach, shards=(), kind=jnp.bfloat16):
    drawn = width * jax.random.normal(own_key, dims, jnp.float32)
    if shards:
        drawn = drawn * shard_levels(own_key, dims, shards, -0.22, 0.18)
    return jnp.clip(drawn, -reach, reach).astype(kind)


def setup_inputs(seed: int = 0, part: int = 0) -> dict:
    splits = jax.random.split(jax.random.key(seed), 15)
    part_keys = jax.random.split(jax.random.fold_in(splits[14], part), 15)
    return {
        "hidden_in": normal_values(part_keys[0], (TOKENS, D), 1.0, 6.0, ((0, 8),)),
        "ffn_gain": jnp.clip(1.0 + 0.1 * jax.random.normal(splits[1], (D,), jnp.float32), 0.5, 1.5).astype(jnp.bfloat16),
        "wi_gate": normal_values(splits[2], (D, FF), D ** -0.5, 0.1875, ((0, 8), (1, 2))),
        "wi_up": normal_values(splits[3], (D, FF), D ** -0.5, 0.1875, ((0, 8), (1, 2))),
        "wo_down": normal_values(splits[4], (FF, D), FF ** -0.5, 0.109375, ((0, 2), (1, 8))),
        "final_gain": jnp.clip(1.0 + 0.1 * jax.random.normal(splits[5], (D,), jnp.float32), 0.5, 1.5).astype(jnp.bfloat16),
        "key_w": normal_values(splits[6], (D, D), D ** -0.5, 0.1875, ((0, 8), (1, 2))),
        "value_w": normal_values(splits[7], (D, D), D ** -0.5, 0.1875, ((0, 8), (1, 2))),
        "query_w": draw_query_w(jax.random.fold_in(splits[14], 71), part),
        "out_w": normal_values(splits[9], (D, D), D ** -0.5, 0.1875, ((0, 2), (1, 8))),
        "dec_gain": jnp.clip(1.0 + 0.1 * jax.random.normal(splits[10], (D,), jnp.float32), 0.5, 1.5).astype(jnp.bfloat16),
        "embed": normal_values(splits[11], (VOCAB, D), 1.0, 6.0, ((0, 8),)),
        "lengths": set_ends(jax.random.randint(part_keys[12], (PASSAGES,), SEG // 5, SEG + 1), jax.random.fold_in(part_keys[12], 1), SEG // 5, SEG).astype(jnp.int32),
        "answer_ids": set_ends(jax.random.randint(part_keys[13], (QUEST, ANS), 0, VOCAB), jax.random.fold_in(part_keys[13], 1), 0, VOCAB - 1).astype(jnp.int32),
    }


EPS = 1e-06
FLOOR = -1e+30

def rms_scale(values, gain):
    mean_square = lax.optimization_barrier(jnp.mean(values * values, axis=-1, keepdims=True))
    return values * lax.rsqrt(mean_square + EPS) * gain.astype(jnp.float32)

def reference(hidden_in, ffn_gain, wi_gate, wi_up, wo_down, final_gain, key_w, value_w, query_w, out_w, dec_gain, embed, lengths, answer_ids):

    def encode(block):
        resid_in = block.astype(jnp.float32)
        enc_in = rms_scale(resid_in, ffn_gain).astype(jnp.bfloat16)
        gate = jnp.dot(enc_in, wi_gate, preferred_element_type=jnp.float32)
        up = jnp.dot(enc_in, wi_up, preferred_element_type=jnp.float32)
        inner = (jax.nn.gelu(gate, approximate=True) * up).astype(jnp.bfloat16)
        resid = resid_in + jnp.dot(inner, wo_down, preferred_element_type=jnp.float32)
        memory = rms_scale(resid, final_gain).astype(jnp.bfloat16)
        keys = jnp.dot(memory, key_w, preferred_element_type=jnp.float32).astype(jnp.bfloat16)
        values = jnp.dot(memory, value_w, preferred_element_type=jnp.float32).astype(jnp.bfloat16)
        return (memory, keys, values)
    blocks = hidden_in.reshape(PASSAGES, SEG, D)
    memory, keys, values = lax.map(encode, blocks)
    flat_ids = answer_ids.reshape(QROWS)
    embedded = jnp.take(embed, flat_ids, axis=0)
    dec_in = rms_scale(embedded.astype(jnp.float32), dec_gain).astype(jnp.bfloat16)
    query = jnp.dot(dec_in, query_w, preferred_element_type=jnp.float32).astype(jnp.bfloat16)
    query_four = query.reshape(QUEST, ANS, HEADS, HEAD_DIM).astype(jnp.float32)
    keys_four = keys.reshape(QUEST, PER_Q * SEG, HEADS, HEAD_DIM).astype(jnp.float32)
    values_four = values.reshape(QUEST, PER_Q * SEG, HEADS, HEAD_DIM).astype(jnp.float32)
    position = jnp.arange(SEG, dtype=jnp.int32)
    live = (position[None, :] < lengths[:, None]).reshape(QUEST, PER_Q * SEG)
    scores = jnp.einsum('qahd,qkhd->qahk', query_four, keys_four, precision=lax.Precision.HIGHEST) * (1.0 / math.sqrt(HEAD_DIM))
    scores = jnp.where(live[:, None, None, :], scores, FLOOR)
    weights = jax.nn.softmax(scores, axis=-1)
    attended = jnp.einsum('qahk,qkhd->qahd', weights, values_four, precision=lax.Precision.HIGHEST)
    attended = attended.reshape(QROWS, D).astype(jnp.bfloat16)
    decoded = embedded.astype(jnp.float32) + jnp.dot(attended, out_w, preferred_element_type=jnp.float32)
    return (memory.reshape(TOKENS, D), decoded.astype(jnp.bfloat16))
```

```python
import math

import jax
import jax.numpy as jnp
from jax import lax
from jax.sharding import PartitionSpec as P

HEAD_DIM = 64
QUEST = 4


EPS = 1e-06
FLOOR = -1e30


def swap(values, axis, distance=1):
    pairs = [(i, i ^ distance) for i in range(lax.axis_size(axis))]
    return jax.tree.map(lambda a: lax.ppermute(a, axis, pairs), values)


def ordered(bit, own, other, dim):
    first = jnp.where(bit == 0, own, other)
    second = jnp.where(bit == 0, other, own)
    return jnp.concatenate([first, second], axis=dim)


def part(values, index, count, dim):
    size = values.shape[dim] // count
    return lax.dynamic_slice_in_dim(values, index * size, size, dim)


def line_gather(block, place, count):
    size = lax.axis_size("wide")
    stride = size // count
    if count > 8:
        groups = [[i * stride + j for i in range(count)] for j in range(stride)]
        return lax.all_gather(block, "wide", axis_index_groups=groups)
    up = [(i, i + stride) for i in range(size - stride)]
    down = [(i + stride, i) for i in range(size - stride)]
    below, above = [], []
    from_below = from_above = block
    for _ in range(count - 1):
        from_below = lax.ppermute(from_below, "wide", up)
        from_above = lax.ppermute(from_above, "wide", down)
        below.insert(0, from_below)
        above.append(from_above)
    return lax.dynamic_slice_in_dim(
        jnp.stack(below + [block] + above), count - 1 - place, count, 0
    )


def rms_scale(values, gain):
    mean_square = jnp.mean(values * values, axis=-1, keepdims=True)
    return values * lax.rsqrt(mean_square + EPS) * gain.astype(jnp.float32)


def add_rows(left, piece):
    return jnp.dot(left, piece, preferred_element_type=jnp.float32)


def join_partial(first, second):
    top = jnp.maximum(first[0], second[0])
    factor_first = jnp.exp(first[0] - top)
    factor_second = jnp.exp(second[0] - top)
    return (
        top,
        first[1] * factor_first + second[1] * factor_second,
        first[2] * factor_first + second[2] * factor_second,
    )


def per_device(
    hidden_in,
    ffn_gain,
    wi_gate,
    wi_up,
    wo_down,
    final_gain,
    key_w,
    value_w,
    query_w,
    out_w,
    dec_gain,
    embed,
    lengths,
    answer_ids,
):
    rows, features = hidden_in.shape
    wide = lax.axis_size("wide")
    group, place, core = (lax.axis_index(a) for a in ("groups", "wide", "narrow"))
    side, pair = place % 2, place // 2
    pairs = wide // 2
    quarters = 2 * lax.axis_size("groups")
    lanes = 128

    def for_side(target, pieces):
        quarter = target * (quarters // 2) + group
        return jnp.concatenate(
            [part(a, quarter, quarters, dim).reshape(-1, lanes) for a, dim in pieces]
        )

    def paired(pieces):
        own = for_side(side, pieces)
        other = swap(for_side(1 - side, pieces), "wide")
        return ordered(side, own[None], other[None], 0)

    def gathered(both):
        return line_gather(both, pair, pairs).reshape(wide, *both.shape[1:])

    hidden_units = wi_gate.shape[1] // quarters
    depth = wi_gate.shape[0]
    ffn = gathered(paired(((wi_gate.T, 0), (wi_up.T, 0), (wo_down, 0))))
    ffn = ffn.reshape(wide, 3, hidden_units, depth).transpose(1, 2, 0, 3)
    gate_t, up_t, down = ffn.reshape(3, hidden_units, features)

    def over_plane(own):
        couple = jnp.concatenate([own, swap(own, "wide")])
        return jnp.concatenate([couple, swap(couple, "groups")])

    def both_halves(own):
        return ordered(core, own, swap(own, "narrow"), 1)

    answers = answer_ids.shape[1]
    per_question = wide // QUEST
    qrows = answer_ids.shape[0] * answers
    vocab_rows = embed.shape[0]
    local_ids = answer_ids.reshape(qrows) - place * vocab_rows
    onehot = (local_ids[:, None] == jnp.arange(vocab_rows, dtype=jnp.int32)[None, :]).astype(
        jnp.bfloat16
    )
    found = jnp.dot(onehot, embed, preferred_element_type=jnp.float32).astype(jnp.bfloat16)
    found = part(found, core, 2, 1)
    distance = wide // 2
    while distance:
        if distance >= per_question:
            bit = place // distance % 2
            found = part(found, bit, 2, 0) + swap(part(found, 1 - bit, 2, 0), "wide", distance)
        else:
            found = found + swap(found, "wide", distance)
        distance //= 2
    embedded_half = found.astype(jnp.float32)
    dec_own = rms_scale(both_halves(found).astype(jnp.float32), dec_gain).astype(jnp.bfloat16)
    dec_in = jnp.concatenate([dec_own, swap(dec_own, "groups")])

    columns = key_w.shape[1] // quarters
    att_pair = paired(((key_w, 1), (value_w, 1), (query_w, 1), (out_w, 0)))
    lengths_all = over_plane(lengths)

    resid_in = hidden_in.astype(jnp.float32)
    enc_own = rms_scale(resid_in, ffn_gain).astype(jnp.bfloat16)
    enc_in = both_halves(over_plane(part(enc_own, core, 2, 1)))
    enc_in, dec_in, lengths_all, att_pair, embedded_half = lax.optimization_barrier(
        (enc_in, dec_in, lengths_all, att_pair, embedded_half)
    )
    contract_last = (((1,), (1,)), ((), ()))
    gate = lax.dot_general(enc_in, gate_t, contract_last, preferred_element_type=jnp.float32)
    up = lax.dot_general(enc_in, up_t, contract_last, preferred_element_type=jnp.float32)
    inner = (jax.nn.gelu(gate, approximate=True) * up).astype(jnp.bfloat16)
    sent_half = add_rows(inner, part(down, 1 - core, 2, 1))
    received_half = swap(sent_half, "narrow")
    sums = add_rows(inner, part(down, core, 2, 1)) + received_half

    def keep_half(values):
        return part(values, core, 2, 1) + swap(part(values, 1 - core, 2, 1), "narrow")

    blocks = sums.reshape(4, rows, -1)
    middle = blocks.shape[2] // 2
    early, late = blocks[:, :, :middle], blocks[:, :, middle:]
    early = early[:2] + swap(early[2:], "groups")
    late = late[::2] + swap(late[1::2], "wide")
    early = early[0] + swap(early[1], "wide")
    late = late[0] + swap(late[1], "groups")
    share = jnp.concatenate([early, late], axis=1)
    resid_half = part(resid_in, core, 2, 1) + share
    own_squares = jnp.sum(resid_half * resid_half, axis=1)
    squares = (own_squares + swap(own_squares, "narrow"))[:, None]
    gain_half = part(final_gain, core, 2, 0).astype(jnp.float32)
    memory_half = (resid_half * lax.rsqrt(squares / features + EPS) * gain_half).astype(
        jnp.bfloat16
    )
    memory_early, memory_late = memory_half[:, :middle], memory_half[:, middle:]
    twin = jnp.stack([memory_late, swap(memory_late, "groups")])
    late_all = jnp.stack([twin, swap(twin, "wide")], axis=1).reshape(4 * rows, middle)
    early_all = over_plane(memory_early)
    early_other, late_other = swap(early_all, "narrow"), swap(late_all, "narrow")
    other_half = jnp.concatenate([early_other[:rows], late_other[:rows]], axis=1)
    memory = ordered(core, memory_half, other_half, 1)

    att = gathered(att_pair)
    att = att.reshape(wide, 4, -1)
    key_q, value_q, query_q = (att[:, i].reshape(features, columns) for i in range(3))
    out_q = att[:, 3].reshape(wide, columns, depth).transpose(1, 0, 2).reshape(columns, features)

    def project(weight):
        own, other = part(weight, core, 2, 0), part(weight, 1 - core, 2, 0)
        return (
            add_rows(early_all, own[:middle])
            + add_rows(late_all, own[middle:])
            + add_rows(early_other, other[:middle])
            + add_rows(late_other, other[middle:])
        ).astype(jnp.bfloat16)

    heads = columns // HEAD_DIM
    keys = project(key_q).reshape(2, 2 * rows, columns)
    values = project(value_q).reshape(2, 2 * rows, columns).astype(jnp.float32)
    query = add_rows(dec_in, query_q).astype(jnp.bfloat16)
    in_head = (
        jnp.arange(columns, dtype=jnp.int32)[None, :] // HEAD_DIM
        == jnp.arange(heads, dtype=jnp.int32)[:, None]
    )[None, :, None, :]
    query_heads = jnp.where(in_head, query.reshape(2, 1, answers, columns), 0)
    scores = jnp.einsum(
        "qhac,qkc->qhak", query_heads, keys, preferred_element_type=jnp.float32
    ) * (1.0 / math.sqrt(HEAD_DIM))
    passage_len = rows // lengths.shape[0]
    live = jnp.arange(passage_len, dtype=jnp.int32)[None, :] < lengths_all[:, None]
    scores = jnp.where(live.reshape(2, 1, 1, 2 * rows), scores, FLOOR)
    top = jnp.max(scores, axis=3, keepdims=True)
    weights = jnp.exp(scores - top)
    total = jnp.sum(weights, axis=3, keepdims=True)
    acc = jnp.einsum("qhak,qkc->qhac", weights, values, precision=lax.Precision.HIGHEST)
    state = (top, total, acc)
    distance = 2
    while distance < per_question:
        state = join_partial(state, swap(state, "wide", distance))
        distance *= 2
    attended = jnp.sum(jnp.where(in_head, state[2] / state[1], 0.0), axis=1)
    attended = attended.astype(jnp.bfloat16).reshape(2 * answers, columns)
    partial_out = keep_half(jnp.dot(attended, out_q, preferred_element_type=jnp.float32))
    share_out = partial_out[:answers] + swap(partial_out[answers:], "groups")
    share_out = share_out + swap(share_out, "wide")
    decoded = (embedded_half + share_out).astype(jnp.bfloat16)
    distance = per_question
    while distance < wide:
        decoded = ordered(place // distance % 2, decoded, swap(decoded, "wide", distance), 0)
        distance *= 2
    return (memory, decoded)


def solution(mesh):
    placed = (
        P(("groups", "wide"), None),
        P(),
        P("wide", "narrow"),
        P("wide", "narrow"),
        P("narrow", "wide"),
        P(),
        P("wide", "narrow"),
        P("wide", "narrow"),
        P("wide", "narrow"),
        P("narrow", "wide"),
        P(),
        P("wide", None),
        P(("groups", "wide")),
        P("groups", None),
    )
    return jax.shard_map(
        per_device,
        mesh=mesh,
        in_specs=placed,
        out_specs=(P(("groups", "wide"), None), P("groups", "narrow")),
        check_vma=False,
    )
```

```python
import math

import jax
import jax.numpy as jnp
from jax import lax
from jax.sharding import PartitionSpec as P

HEAD_DIM = 64
QUEST = 4


EPS = 1e-06
FLOOR = -1e30


def swap(values, axis, distance=1):
    pairs = [(i, i ^ distance) for i in range(lax.axis_size(axis))]
    return jax.tree.map(lambda a: lax.ppermute(a, axis, pairs), values)


def ordered(bit, own, other, dim):
    first = jnp.where(bit == 0, own, other)
    second = jnp.where(bit == 0, other, own)
    return jnp.concatenate([first, second], axis=dim)


def part(values, index, count, dim):
    size = values.shape[dim] // count
    return lax.dynamic_slice_in_dim(values, index * size, size, dim)


def line_gather(block, place, count):
    size = lax.axis_size("wide")
    stride = size // count
    if count > 8:
        groups = [[i * stride + j for i in range(count)] for j in range(stride)]
        return lax.all_gather(block, "wide", axis_index_groups=groups)
    up = [(i, i + stride) for i in range(size - stride)]
    down = [(i + stride, i) for i in range(size - stride)]
    below, above = [], []
    from_below = from_above = block
    for _ in range(count - 1):
        from_below = lax.ppermute(from_below, "wide", up)
        from_above = lax.ppermute(from_above, "wide", down)
        below.insert(0, from_below)
        above.append(from_above)
    return lax.dynamic_slice_in_dim(
        jnp.stack(below + [block] + above), count - 1 - place, count, 0
    )


def rms_scale(values, gain):
    mean_square = jnp.mean(values * values, axis=-1, keepdims=True)
    return values * lax.rsqrt(mean_square + EPS) * gain.astype(jnp.float32)


def add_rows(left, piece):
    return jnp.dot(left, piece, preferred_element_type=jnp.float32)


def join_partial(first, second):
    top = jnp.maximum(first[0], second[0])
    factor_first = jnp.exp(first[0] - top)
    factor_second = jnp.exp(second[0] - top)
    return (
        top,
        first[1] * factor_first + second[1] * factor_second,
        first[2] * factor_first + second[2] * factor_second,
    )


def per_device(
    hidden_in,
    ffn_gain,
    wi_gate,
    wi_up,
    wo_down,
    final_gain,
    key_w,
    value_w,
    query_w,
    out_w,
    dec_gain,
    embed,
    lengths,
    answer_ids,
):
    rows, features = hidden_in.shape
    wide = lax.axis_size("wide")
    group, place, core = (lax.axis_index(a) for a in ("groups", "wide", "narrow"))
    side, pair = place % 2, place // 2
    pairs = wide // 2
    quarters = 2 * lax.axis_size("groups")
    lanes = 128

    def for_side(target, pieces):
        quarter = target * (quarters // 2) + group
        return jnp.concatenate(
            [part(a, quarter, quarters, dim).reshape(-1, lanes) for a, dim in pieces]
        )

    def paired(pieces):
        own = for_side(side, pieces)
        other = swap(for_side(1 - side, pieces), "wide")
        return ordered(side, own[None], other[None], 0)

    def gathered(both):
        return line_gather(both, pair, pairs).reshape(wide, *both.shape[1:])

    hidden_units = wi_gate.shape[1] // quarters
    depth = wi_gate.shape[0]
    ffn = gathered(paired(((wi_gate.T, 0), (wi_up.T, 0), (wo_down, 0))))
    ffn = ffn.reshape(wide, 3, hidden_units, depth).transpose(1, 2, 0, 3)
    gate_t, up_t, down = ffn.reshape(3, hidden_units, features)

    def over_plane(own):
        couple = jnp.concatenate([own, swap(own, "wide")])
        return jnp.concatenate([couple, swap(couple, "groups")])

    def both_halves(own):
        return ordered(core, own, swap(own, "narrow"), 1)

    answers = answer_ids.shape[1]
    per_question = wide // QUEST
    qrows = answer_ids.shape[0] * answers
    vocab_rows = embed.shape[0]
    local_ids = answer_ids.reshape(qrows) - place * vocab_rows
    onehot = (local_ids[:, None] == jnp.arange(vocab_rows, dtype=jnp.int32)[None, :]).astype(
        jnp.bfloat16
    )
    found = jnp.dot(onehot, embed, preferred_element_type=jnp.float32).astype(jnp.bfloat16)
    found = part(found, core, 2, 1)
    distance = wide // 2
    while distance:
        if distance >= per_question:
            bit = place // distance % 2
            found = part(found, bit, 2, 0) + swap(part(found, 1 - bit, 2, 0), "wide", distance)
        else:
            found = found + swap(found, "wide", distance)
        distance //= 2
    embedded_half = found.astype(jnp.float32)
    dec_own = rms_scale(both_halves(found).astype(jnp.float32), dec_gain).astype(jnp.bfloat16)
    dec_in = jnp.concatenate([dec_own, swap(dec_own, "groups")])

    columns = key_w.shape[1] // quarters
    att_pair = paired(((key_w, 1), (value_w, 1), (query_w, 1), (out_w, 0)))
    lengths_all = over_plane(lengths)

    resid_in = hidden_in.astype(jnp.float32)
    enc_own = rms_scale(resid_in, ffn_gain).astype(jnp.bfloat16)
    enc_in = both_halves(over_plane(part(enc_own, core, 2, 1)))
    enc_in, dec_in, lengths_all, att_pair, embedded_half = lax.optimization_barrier(
        (enc_in, dec_in, lengths_all, att_pair, embedded_half)
    )
    contract_last = (((1,), (1,)), ((), ()))
    gate = lax.dot_general(enc_in, gate_t, contract_last, preferred_element_type=jnp.float32)
    up = lax.dot_general(enc_in, up_t, contract_last, preferred_element_type=jnp.float32)
    inner = (jax.nn.gelu(gate, approximate=True) * up).astype(jnp.bfloat16)
    sent_half = add_rows(inner, part(down, 1 - core, 2, 1))
    received_half = swap(sent_half, "narrow")
    sums = add_rows(inner, part(down, core, 2, 1)) + received_half
    sums, att_pair = lax.optimization_barrier((sums, att_pair))

    def keep_half(values):
        return part(values, core, 2, 1) + swap(part(values, 1 - core, 2, 1), "narrow")

    blocks = sums.reshape(4, rows, -1)
    middle = blocks.shape[2] // 2
    early, late = blocks[:, :, :middle], blocks[:, :, middle:]
    early = early[:2] + swap(early[2:], "groups")
    late = late[::2] + swap(late[1::2], "wide")
    early = early[0] + swap(early[1], "wide")
    late = late[0] + swap(late[1], "groups")
    share = jnp.concatenate([early, late], axis=1)
    resid_half = part(resid_in, core, 2, 1) + share
    own_squares = jnp.sum(resid_half * resid_half, axis=1)
    squares = (own_squares + swap(own_squares, "narrow"))[:, None]
    gain_half = part(final_gain, core, 2, 0).astype(jnp.float32)
    memory_half = (resid_half * lax.rsqrt(squares / features + EPS) * gain_half).astype(
        jnp.bfloat16
    )
    memory_early, memory_late = memory_half[:, :middle], memory_half[:, middle:]
    twin = jnp.stack([memory_late, swap(memory_late, "groups")])
    late_all = jnp.stack([twin, swap(twin, "wide")], axis=1).reshape(4 * rows, middle)
    early_all = over_plane(memory_early)
    early_other, late_other = swap(early_all, "narrow"), swap(late_all, "narrow")
    other_half = jnp.concatenate([early_other[:rows], late_other[:rows]], axis=1)
    memory = ordered(core, memory_half, other_half, 1)

    att = gathered(att_pair)
    att = att.reshape(wide, 4, -1)
    key_q, value_q, query_q = (att[:, i].reshape(features, columns) for i in range(3))
    out_q = att[:, 3].reshape(wide, columns, depth).transpose(1, 0, 2).reshape(columns, features)

    def project(weight):
        own, other = part(weight, core, 2, 0), part(weight, 1 - core, 2, 0)
        return (
            add_rows(early_all, own[:middle])
            + add_rows(late_all, own[middle:])
            + add_rows(early_other, other[:middle])
            + add_rows(late_other, other[middle:])
        ).astype(jnp.bfloat16)

    heads = columns // HEAD_DIM
    keys = project(key_q).reshape(2, 2 * rows, columns)
    values = project(value_q).reshape(2, 2 * rows, columns).astype(jnp.float32)
    query = add_rows(dec_in, query_q).astype(jnp.bfloat16)
    in_head = (
        jnp.arange(columns, dtype=jnp.int32)[None, :] // HEAD_DIM
        == jnp.arange(heads, dtype=jnp.int32)[:, None]
    )[None, :, None, :]
    query_heads = jnp.where(in_head, query.reshape(2, 1, answers, columns), 0)
    scores = jnp.einsum(
        "qhac,qkc->qhak", query_heads, keys, preferred_element_type=jnp.float32
    ) * (1.0 / math.sqrt(HEAD_DIM))
    passage_len = rows // lengths.shape[0]
    live = jnp.arange(passage_len, dtype=jnp.int32)[None, :] < lengths_all[:, None]
    scores = jnp.where(live.reshape(2, 1, 1, 2 * rows), scores, FLOOR)
    top = jnp.max(scores, axis=3, keepdims=True)
    weights = jnp.exp(scores - top)
    total = jnp.sum(weights, axis=3, keepdims=True)
    acc = jnp.einsum("qhak,qkc->qhac", weights, values, precision=lax.Precision.HIGHEST)
    state = (top, total, acc)
    distance = 2
    while distance < per_question:
        state = join_partial(state, swap(state, "wide", distance))
        distance *= 2
    attended = jnp.sum(jnp.where(in_head, state[2] / state[1], 0.0), axis=1)
    attended = attended.astype(jnp.bfloat16).reshape(2 * answers, columns)
    partial_out = keep_half(jnp.dot(attended, out_q, preferred_element_type=jnp.float32))
    share_out = partial_out[:answers] + swap(partial_out[answers:], "groups")
    share_out = share_out + swap(share_out, "wide")
    decoded = (embedded_half + share_out).astype(jnp.bfloat16)
    distance = per_question
    while distance < wide:
        decoded = ordered(place // distance % 2, decoded, swap(decoded, "wide", distance), 0)
        distance *= 2
    return (memory, decoded)


def solution(mesh):
    placed = (
        P(("groups", "wide"), None),
        P(),
        P("wide", "narrow"),
        P("wide", "narrow"),
        P("narrow", "wide"),
        P(),
        P("wide", "narrow"),
        P("wide", "narrow"),
        P("wide", "narrow"),
        P("narrow", "wide"),
        P(),
        P("wide", None),
        P(("groups", "wide")),
        P("groups", None),
    )
    return jax.shard_map(
        per_device,
        mesh=mesh,
        in_specs=placed,
        out_specs=(P(("groups", "wide"), None), P("groups", "narrow")),
        check_vma=False,
    )
```
